32 devices in a mesh: dp: 8 (over y, x, core), mp: 4 (over z).
Axes of the slice: x: 2, y: 2, z: 4, core: 2. Of those that a mesh axis runs over, the one named last changes fastest.
Arguments:
- grad_out: bfloat16 [1024, 2688], P('dp', 'mp'), may hold values from -24 to 24
- gate_pre: bfloat16 [1024, 10752], P('dp', 'mp'), may hold values from -6 to 6
- up_pre: bfloat16 [1024, 10752], P('dp', 'mp'), may hold values from -6 to 6
- down_weight: bfloat16 [2688, 10752], P('dp', 'mp'), may hold values from -0.125 to 0.125
- new_logp: float32 [1024], P('dp'), may hold values from -3 to 0
- behav_logp: float32 [1024], P('dp'), may hold values from -3 to 0
- lengths: int32 [8], P('dp'), may hold values from 1 to 128
- versions: int32 [8], P('dp'), may hold values from 0 to 7
- token_lag: int32 [1024], P('dp'), may hold values from 0 to 3
Outputs:
- d_gate: bfloat16 [1024, 10752], P('dp', 'mp')
- d_up: bfloat16 [1024, 10752], P('dp', 'mp')
- d_down: float32 [2688, 10752], P('dp', 'mp')
The draws below stay inside these ranges and needn't reach their ends.
All inputs are finite; a program needn't handle non-finite values.
Results may differ from the reference program's by a relative error of at most 0.017.
Values may be sent and summed in bfloat16 or wider, within the bound.
No kernel may reach another device: no remote copies, remote signals or barrier semaphores. Data moves between devices by JAX's collectives and lax.ppermute only.
A program may use at most 64 MiB of HBM per device.

```python
import jax
import jax.numpy as jnp
from jax import lax

D = 2688
FF = 10752
LEN = 128
SEQ_DEV = 1
VERSIONS = 8
LAGS = 4
MAX_LAG = 5
TOK_DEV = 128
SEQS = 8
TOKENS = 1024


def draw_lengths(key, part):
    seq_index = jnp.arange(SEQS, dtype=jnp.int32)
    groups = SEQS // SEQ_DEV
    spread = max(groups - 1, 1)
    device = seq_index // SEQ_DEV
    highest = LEN * (spread + 2 * device) // (3 * spread)
    highest = jnp.maximum(highest, 2)
    lowest = highest // 2
    random_bits = jax.random.randint(key, (SEQS,), 0, 1 << 20)
    length = lowest + random_bits % (highest - lowest + 1)
    length = jnp.where(seq_index == SEQS - 1, LEN, length)
    return jnp.clip(length, 1, LEN).astype(jnp.int32)


def place_ends(array, stream_key, low, largest):
    shape = array.shape
    place = [jax.random.randint(jax.random.fold_in(stream_key, axis), (), 0, shape[axis]) for axis in range(len(shape))]
    array = array.at[tuple(place)].set(low)
    longest = shape.index(max(shape))
    place[longest] = (place[longest] + 1) % shape[longest]
    return array.at[tuple(place)].set(largest)


def strengthened(entries, rng, source, target, blocks, factor):
    owner, partner = [(jnp.arange(entries.shape[axis_at]) // (entries.shape[axis_at] // blocks)).reshape([-1 if axis == axis_at else 1 for axis in range(entries.ndim)]) for axis_at in (source, target)]
    chosen = jax.random.permutation(rng, blocks)[partner]
    strong = (owner == chosen) | (owner == (partner + blocks // 2) % blocks)
    return jnp.where(strong, factor * entries, entries)


def block_scale(own_key, dims, pieces, low, high):
    gain, own = 1.0, jax.random.fold_in(own_key, 6)
    for dim, blocks in pieces:
        steps = jnp.exp(jax.random.uniform(jax.random.fold_in(own, dim), (blocks,), jnp.float32, low / len(pieces), high / len(pieces)))
        gain = gain * jnp.repeat(steps, dims[dim] // blocks).reshape([-1 if axis == dim else 1 for axis in range(len(dims))])
    return gain


def normal_values(stream_key, shape, deviation, limit, shards=(), kind=jnp.bfloat16):
    array = deviation * jax.random.normal(stream_key, shape, jnp.float32)
    if shards:
        array = array * block_scale(stream_key, shape, shards, -0.22, 0.18)
    return jnp.clip(array, -limit, limit).astype(kind)


def noise_with(key, shape, width, most, shards, heavy, kind=jnp.bfloat16):
    result = width * jax.random.normal(key, shape, jnp.float32)
    if shards:
        result = result * block_scale(key, shape, shards, -0.22, 0.18)
    return jnp.clip(strengthened(result, jax.random.fold_in(key, 3), *heavy), -most, most).astype(kind)


def setup_inputs(seed: int = 0) -> dict:
    arg_keys = jax.random.split(jax.random.key(seed), 10)
    return {
        "grad_out": noise_with(arg_keys[0], (TOKENS, D), 4.0, 24.0, ((0, 8), (1, 4)), (0, 1, 8, 2.0)),
        "gate_pre": normal_values(arg_keys[1], (TOKENS, FF), 1.0, 6.0, ((0, 8), (1, 4))),
        "up_pre": normal_values(arg_keys[2], (TOKENS, FF), 1.0, 6.0, ((0, 8), (1, 4))),
        "down_weight": normal_values(arg_keys[3], (D, FF), D ** -0.5, 0.125, ((0, 8), (1, 4))),
        "new_logp": jnp.clip(-3.0 + 3.0 * jax.random.uniform(arg_keys[4], (TOKENS,), jnp.float32) ** block_scale(arg_keys[4], (TOKENS,), ((0, 8),), -0.2, 0.2), -3.0, 0.0),
        "behav_logp": jnp.clip(-3.0 + 3.0 * jax.random.uniform(arg_keys[5], (TOKENS,), jnp.float32) ** block_scale(arg_keys[5], (TOKENS,), ((0, 8),), -0.2, 0.2), -3.0, 0.0),
        "lengths": draw_lengths(jax.random.fold_in(arg_keys[9], 71), 0),
        "versions": place_ends(jax.random.randint(arg_keys[7], (SEQS,), 0, VERSIONS), jax.random.fold_in(arg_keys[7], 1), 0, VERSIONS - 1).astype(jnp.int32),
        "token_lag": place_ends(jax.random.randint(arg_keys[8], (TOKENS,), 0, LAGS), jax.random.fold_in(arg_keys[8], 1), 0, LAGS - 1).astype(jnp.int32),
    }


ratio_cap = 2.0


def gelu_tanh(values):
    return jax.nn.gelu(values, approximate=True)


def reference(grad_out, gate_pre, up_pre, down_weight, new_logp, behav_logp, lengths, versions, token_lag):
    token_ids = jnp.arange(TOKENS, dtype=jnp.int32)
    positions = token_ids % LEN
    seq_of = token_ids // LEN
    in_length = positions < lengths[seq_of]
    token_version = versions[seq_of] + token_lag
    current = jnp.max(jnp.where(in_length, token_version, -1))
    is_valid = in_length & (token_version >= current - MAX_LAG)
    valid_count = jnp.sum(is_valid.astype(jnp.float32))
    ratios = jnp.minimum(jnp.exp(new_logp - behav_logp), ratio_cap)
    weights = jnp.where(is_valid, ratios, jnp.float32(0.0)) * (SEQS / valid_count)
    scaled = (weights[:, None] * grad_out.astype(jnp.float32)).astype(jnp.bfloat16)
    gate = gate_pre.astype(jnp.float32)
    upper = up_pre.astype(jnp.float32)
    activated, slope = jax.jvp(gelu_tanh, (gate,), (jnp.ones_like(gate),))
    hidden = (activated * upper).astype(jnp.bfloat16)
    blocks = SEQS // SEQ_DEV
    scaled_blocks = scaled.reshape(blocks, TOK_DEV, D)
    hidden_blocks = hidden.reshape(blocks, TOK_DEV, FF)

    def add_block(total, pair):
        partial_sum = lax.dot_general(pair[0], pair[1], (((0,), (0,)), ((), ())), preferred_element_type=jnp.float32)
        rounded = lax.optimization_barrier(partial_sum.astype(jnp.bfloat16))
        return total + rounded.astype(jnp.float32), None

    d_down, unused = lax.scan(add_block, jnp.zeros((D, FF), jnp.float32), (scaled_blocks, hidden_blocks))
    d_hidden = jnp.dot(scaled, down_weight, preferred_element_type=jnp.float32)
    d_up = (d_hidden * activated).astype(jnp.bfloat16)
    d_gate = (d_hidden * upper * slope).astype(jnp.bfloat16)
    return d_gate, d_up, d_down
```

```python
import jax
import jax.numpy as jnp
from jax import lax
from jax.sharding import PartitionSpec as P

MAX_LAG = 5
RATIO_CAP = 2.0
INFO_ROWS = 16
F32 = jnp.float32
BF16 = jnp.bfloat16


def gelu_tanh(values):
    return jax.nn.gelu(values, approximate=True)


def bf16_part(value):
    return lax.reduce_precision(value, 8, 7)


def swap(array, bit):
    size = lax.axis_size("dp")
    return lax.ppermute(array, "dp", [(i, i ^ bit) for i in range(size)])


def colours(dp):
    chip_bits = [1 << k for k in range(1, dp.bit_length() - 1)]
    half = len(chip_bits) // 2
    return (chip_bits, chip_bits[half:] + chip_bits[:half])


def redistribute(grad_out, info, dp, mp):
    rows = grad_out.shape[1] * mp // dp
    group = dp // mp
    low = lax.axis_index("dp") % group
    features = grad_out.T.reshape(group, rows, grad_out.shape[0])
    pieces = jnp.concatenate(
        [features, jnp.broadcast_to(info[None], (group,) + info.shape)], axis=1
    )
    received = [None] * dp
    for step_low in range(group):
        piece = lax.dynamic_index_in_dim(pieces, low ^ step_low, 0, keepdims=False)
        for step_high in range(mp):
            perm = []
            for source in range(dp):
                for column in range(mp):
                    target = group * column + ((source % group) ^ step_low)
                    plane = (source // group) ^ step_high
                    perm.append((source * mp + column, target * mp + plane))
            received[group * step_high + step_low] = lax.ppermute(piece, ("dp", "mp"), perm)
    return received


def local(
    grad_out, gate_pre, up_pre, down_weight, new_logp, behav_logp, lengths, versions, token_lag
):
    dp, mp = lax.axis_size("dp"), lax.axis_size("mp")
    group = dp // mp
    tokens = token_lag.shape[0]
    seqs = lengths.shape[0]
    seq_len = tokens // seqs
    rows = down_weight.shape[0]
    me, plane = lax.axis_index("dp"), lax.axis_index("mp")

    positions = jnp.arange(seq_len, dtype=jnp.int32)
    in_length = (positions[None, :] < lengths[:, None]).reshape(tokens)
    version = (versions[:, None] + token_lag.reshape(seqs, seq_len)).reshape(tokens)
    version = jnp.where(in_length, version, -1).astype(F32)
    ratios = jnp.minimum(jnp.exp(new_logp - behav_logp), RATIO_CAP)
    high = bf16_part(ratios)
    middle = bf16_part(ratios - high)
    lowest = ratios - high - middle
    info = jnp.stack([high, middle, lowest, version]).astype(BF16)
    info = jnp.pad(info, ((0, INFO_ROWS - 4), (0, 0)))

    received = jnp.stack(redistribute(grad_out, info, dp, mp))

    gate = gate_pre.astype(F32)
    upper = up_pre.astype(F32)
    activated, slope = jax.jvp(gelu_tanh, (gate,), (jnp.ones_like(gate),))
    hidden = (activated * upper).astype(BF16)

    half = tokens // 2
    orders = colours(dp)
    gathered = []
    for colour, order in enumerate(orders):
        have = {0: lax.slice_in_dim(hidden, colour * half, (colour + 1) * half)}
        for bit in order:
            have.update({mask ^ bit: swap(block, bit) for mask, block in have.items()})
        have.update({mask ^ 1: swap(block, 1) for mask, block in have.items()})
        gathered.append(have)

    masks = list(range(1, dp, 2)) + list(range(0, dp, 2))
    delta = group * (plane ^ (me // group))
    blocks = [
        lax.dynamic_index_in_dim(received, delta ^ mask, 0, keepdims=False) for mask in masks
    ]
    every = jnp.concatenate(blocks, axis=1)
    part = every[rows : rows + 4].astype(F32)
    ratio = part[0] + part[1] + part[2]
    token_version = part[3]
    current = jnp.max(token_version)
    is_valid = (token_version >= 0) & (token_version >= current - MAX_LAG)
    valid_count = jnp.sum(is_valid.astype(F32))
    weights = jnp.where(is_valid, ratio, F32(0.0)) * (seqs * dp / valid_count)
    scaled = (every[:rows].astype(F32) * weights[None, :]).astype(BF16)

    count = len(masks) // 2 * tokens

    def partial_of(columns):
        return lax.dot_general(
            columns, down_weight, (((0,), (0,)), ((), ())), preferred_element_type=F32
        ).astype(BF16)

    outgoing = swap(partial_of(scaled[:, :count]), 1)
    kept = partial_of(scaled[:, count:])
    even = masks[len(masks) // 2 :]
    summed = []
    for colour, order in enumerate(orders):
        current_sum = {}
        for place, mask in enumerate(even):
            start = place * tokens + colour * half
            current_sum[mask] = (
                lax.slice_in_dim(kept, start, start + half).astype(F32)
                + lax.slice_in_dim(outgoing, start, start + half).astype(F32)
            )
        for bit in order:
            arrived = {
                mask ^ bit: swap(value.astype(BF16), bit)
                for mask, value in current_sum.items()
                if mask & bit
            }
            current_sum = {
                mask: value + arrived[mask].astype(F32)
                for mask, value in current_sum.items()
                if not mask & bit
            }
        summed.append(current_sum[0])
    d_hidden = jnp.concatenate(summed, axis=0)

    all_hidden = jnp.concatenate(
        [gathered[colour][mask] for mask in masks for colour in range(2)], axis=0
    )
    d_down = jnp.dot(scaled, all_hidden, preferred_element_type=F32)
    d_up = (d_hidden * activated).astype(BF16)
    d_gate = (d_hidden * upper * slope).astype(BF16)
    return (d_gate, d_up, d_down)


def solution(mesh):
    in_specs = (
        P("dp", "mp"),
        P("dp", "mp"),
        P("dp", "mp"),
        P("dp", "mp"),
        P("dp"),
        P("dp"),
        P("dp"),
        P("dp"),
        P("dp"),
    )
    out_specs = (P("dp", "mp"), P("dp", "mp"), P("dp", "mp"))
    return jax.shard_map(local, mesh=mesh, in_specs=in_specs, out_specs=out_specs, check_vma=False)
```
